8 devices in a mesh: pod: 1 (over z), dp: 2 (over y), tp: 4 (over x, core).
Axes of the slice: x: 2, y: 2, z: 1, core: 2. Of those that a mesh axis runs over, the one named last changes fastest.
Arguments:
- hidden: bfloat16 [2, 2048, 2304], P(('pod', 'dp'), 'tp')
- out_grad: bfloat16 [2, 2048, 2304], P(('pod', 'dp'), 'tp')
- gain_attn: float32 [2, 2304], replicated
- w_qkv: bfloat16 [2, 2304, 4, 1024], P(None, None, 'tp')
- w_out: bfloat16 [2, 2048, 2304], P(None, 'tp')
- gain_mlp: float32 [2, 2304], replicated
- w_gate: bfloat16 [2, 2304, 9216], P(None, None, 'tp')
- w_up: bfloat16 [2, 2304, 9216], P(None, None, 'tp')
- w_down: bfloat16 [2, 9216, 2304], P(None, 'tp')
Outputs:
- output 1: bfloat16 [2, 2048, 2304], P(('pod', 'dp'), 'tp')
- output 2: float32 [2, 2304], P('pod')
- output 3: bfloat16 [2, 2304, 4, 1024], P('pod', None, 'tp', 'dp')
- output 4: bfloat16 [2, 2048, 2304], P('pod', ('tp', 'dp'))
- output 5: float32 [2, 2304], P('pod')
- output 6: bfloat16 [2, 2304, 9216], P('pod', None, ('tp', 'dp'))
- output 7: bfloat16 [2, 2304, 9216], P('pod', None, ('tp', 'dp'))
- output 8: bfloat16 [2, 9216, 2304], P('pod', ('tp', 'dp'))
All inputs are finite; a program needn't handle non-finite values.
Results may differ from the reference program's by a relative error of at most 0.02.
Values are sent between devices in bfloat16 or wider.
A program may use at most 1 GiB of HBM per device.

```python
import math
import jax
import jax.numpy as jnp
from jax import lax

DATA_WAYS = 2
TP_WAYS = 4
SEQ_DEV = 512
LAYERS = 2
D_MODEL = 2304
HEADS = 8
KV_HEADS = 4
HEAD_DIM = 256
FF_DIM = 9216

SEQ_LEN = SEQ_DEV * TP_WAYS
GROUP_SIZE = HEADS // KV_HEADS
GROUP_COLS = (GROUP_SIZE + 2) * HEAD_DIM
NORM_EPS = 1e-5
MASK_FILL = -1e30


def setup_inputs(seed: int = 0, part: int = 0) -> dict:
    base_key = jax.random.key(seed)
    key_x, key_g = jax.random.split(jax.random.fold_in(base_key, part))
    key_list = jax.random.split(base_key, 8)
    qk_gain = math.log(SEQ_LEN / 8.0) ** 0.125
    col_gain = jnp.repeat(jnp.where(jnp.arange(GROUP_SIZE + 2) <= GROUP_SIZE, qk_gain, 1.0), HEAD_DIM)
    act_shape = (DATA_WAYS, SEQ_LEN, D_MODEL)
    hidden = jax.random.normal(key_x, act_shape, jnp.float32)
    out_grad = jax.random.normal(key_g, act_shape, jnp.float32)
    gain_attn = 1.0 + 0.3 * jax.random.normal(key_list[0], (LAYERS, D_MODEL), jnp.float32)
    gain_mlp = 1.0 + 0.3 * jax.random.normal(key_list[1], (LAYERS, D_MODEL), jnp.float32)
    w_qkv = jax.random.normal(key_list[2], (LAYERS, D_MODEL, KV_HEADS, GROUP_COLS), jnp.float32) * col_gain * D_MODEL ** -0.5
    w_out = jax.random.normal(key_list[3], (LAYERS, HEADS * HEAD_DIM, D_MODEL), jnp.float32) * (HEADS * HEAD_DIM) ** -0.5
    w_gate = jax.random.normal(key_list[4], (LAYERS, D_MODEL, FF_DIM), jnp.float32) * D_MODEL ** -0.5
    w_up = jax.random.normal(key_list[5], (LAYERS, D_MODEL, FF_DIM), jnp.float32) * D_MODEL ** -0.5
    w_down = jax.random.normal(key_list[6], (LAYERS, FF_DIM, D_MODEL), jnp.float32) * FF_DIM ** -0.5
    return dict(hidden=hidden.astype(jnp.bfloat16), out_grad=out_grad.astype(jnp.bfloat16), gain_attn=gain_attn, w_qkv=w_qkv.astype(jnp.bfloat16), w_out=w_out.astype(jnp.bfloat16), gain_mlp=gain_mlp, w_gate=w_gate.astype(jnp.bfloat16), w_up=w_up.astype(jnp.bfloat16), w_down=w_down.astype(jnp.bfloat16))


def rms_scale(values_in, gain_row):
    values_f = values_in.astype(jnp.float32)
    inv_rms = lax.rsqrt(jnp.mean(values_f * values_f, axis=-1, keepdims=True) + NORM_EPS)
    return (values_f * inv_rms * gain_row).astype(jnp.bfloat16)


def attend_group(group_qkv):
    query_rows = group_qkv[:, :GROUP_SIZE].astype(jnp.float32)
    key_rows = group_qkv[:, GROUP_SIZE].astype(jnp.float32)
    value_rows = group_qkv[:, GROUP_SIZE + 1].astype(jnp.float32)
    scores = jnp.einsum('sgd,td->gst', query_rows, key_rows) * HEAD_DIM ** -0.5
    causal = jnp.arange(SEQ_LEN)[:, None] >= jnp.arange(SEQ_LEN)[None, :]
    scores = jnp.where(causal, scores, MASK_FILL)
    prob_rows = jax.nn.softmax(scores, axis=-1).astype(jnp.bfloat16).astype(jnp.float32)
    return jnp.einsum('gst,td->sgd', prob_rows, value_rows).astype(jnp.bfloat16)


def layer_forward(resid, params):
    gain_attn, w_qkv, w_out, gain_mlp, w_gate, w_up, w_down = params
    tokens = DATA_WAYS * SEQ_LEN
    resid_rows = resid.reshape(tokens, D_MODEL)
    normed = rms_scale(resid_rows, gain_attn)
    qkv_rows = jnp.dot(normed, w_qkv.reshape(D_MODEL, KV_HEADS * GROUP_COLS), preferred_element_type=jnp.float32).astype(jnp.bfloat16)
    grouped = qkv_rows.reshape(DATA_WAYS, SEQ_LEN, KV_HEADS, GROUP_SIZE + 2, HEAD_DIM).transpose(0, 2, 1, 3, 4)
    context = lax.map(jax.checkpoint(attend_group), grouped.reshape(DATA_WAYS * KV_HEADS, SEQ_LEN, GROUP_SIZE + 2, HEAD_DIM))
    context = context.reshape(DATA_WAYS, KV_HEADS, SEQ_LEN, GROUP_SIZE, HEAD_DIM).transpose(0, 2, 1, 3, 4).reshape(tokens, HEADS * HEAD_DIM)
    mid_resid = (resid_rows.astype(jnp.float32) + jnp.dot(context, w_out, preferred_element_type=jnp.float32)).astype(jnp.bfloat16)
    normed_mlp = rms_scale(mid_resid, gain_mlp)
    gate_pre = jnp.dot(normed_mlp, w_gate, preferred_element_type=jnp.float32)
    up_pre = jnp.dot(normed_mlp, w_up, preferred_element_type=jnp.float32)
    hidden_act = (jax.nn.silu(gate_pre) * up_pre).astype(jnp.bfloat16)
    out_rows = (mid_resid.astype(jnp.float32) + jnp.dot(hidden_act, w_down, preferred_element_type=jnp.float32)).astype(jnp.bfloat16)
    return out_rows.reshape(DATA_WAYS, SEQ_LEN, D_MODEL)


def stack_forward(hidden, gain_attn, w_qkv, w_out, gain_mlp, w_gate, w_up, w_down):
    def layer_step(resid, params):
        return jax.checkpoint(layer_forward)(resid, params), None
    stack_out, _ = lax.scan(layer_step, hidden, (gain_attn, w_qkv, w_out, gain_mlp, w_gate, w_up, w_down))
    return stack_out


def reference(hidden, out_grad, gain_attn, w_qkv, w_out, gain_mlp, w_gate, w_up, w_down):
    _, pullback = jax.vjp(stack_forward, hidden, gain_attn, w_qkv, w_out, gain_mlp, w_gate, w_up, w_down)
    grad_list = pullback(out_grad)
    return (grad_list[0], grad_list[1], grad_list[2], grad_list[3], grad_list[4], grad_list[5], grad_list[6], grad_list[7])
```

```python
import functools
import jax
import jax.numpy as jnp
from jax import lax
from jax.experimental import pallas as pl
from jax.experimental.pallas import tpu as pltpu
from jax.sharding import PartitionSpec as P


NORM_EPS = 1e-5
MASK_FILL = -1e30
BLOCK = 512
FWD_CHUNKS = 2
ACT_SPEC = P(('pod', 'dp'), 'tp', None)
IN_SPECS = (ACT_SPEC, ACT_SPEC, P(None, None), P(None, None, 'tp', None), P(None, 'tp', None), P(None, None), P(None, None, 'tp'), P(None, None, 'tp'), P(None, 'tp', None))
OUT_SPECS = (ACT_SPEC, P('pod', None), P('pod', None, 'tp', 'dp'), P('pod', ('tp', 'dp'), None), P('pod', None), P('pod', None, ('tp', 'dp')), P('pod', None, ('tp', 'dp')), P('pod', ('tp', 'dp'), None))

NN = (((1,), (0,)), ((), ()))
NT = (((1,), (1,)), ((), ()))
TN = (((0,), (0,)), ((), ()))


def mm(a, b, dims=NN):
    return lax.dot_general(a, b, dims, preferred_element_type=jnp.float32)


def rms_forward(values_in, gain_row):
    values_f = values_in.astype(jnp.float32)
    inv_rms = lax.rsqrt(jnp.mean(values_f * values_f, axis=-1, keepdims=True) + NORM_EPS)
    return (values_f * inv_rms * gain_row).astype(jnp.bfloat16), inv_rms


def rms_backward(grad_normed, values_in, inv_rms, gain_row):
    unit_rows = values_in.astype(jnp.float32) * inv_rms
    grad_unit = grad_normed * gain_row
    grad_values = inv_rms * (grad_unit - unit_rows * jnp.mean(grad_unit * unit_rows, axis=-1, keepdims=True))
    return grad_values, jnp.sum(grad_normed * unit_rows, axis=0)


def causal_fill(scores_t):
    keys = lax.broadcasted_iota(jnp.int32, scores_t.shape, 0)
    queries = lax.broadcasted_iota(jnp.int32, scores_t.shape, 1)
    return jnp.where(queries >= keys, scores_t, MASK_FILL)


def attention_forward_kernel(scale, q_ref, k_ref, v_ref, ctx_ref, lse_ref, vt_ref, s_ref):
    head, qi = pl.program_id(0), pl.program_id(1)

    @pl.when((head == 0) & (qi == 0))
    def _():
        vt_ref[...] = v_ref[...].T

    q = q_ref[...]

    def score(j, top, diagonal):
        rows = pl.ds(pl.multiple_of(j * BLOCK, BLOCK), BLOCK)
        s = mm(k_ref[rows, :], q, NT) * scale
        if diagonal:
            s = causal_fill(s)
        s_ref[rows, :] = s
        return jnp.maximum(top, jnp.max(s, axis=0, keepdims=True))

    top = lax.fori_loop(0, qi, lambda j, t: score(j, t, False), jnp.full((1, BLOCK), MASK_FILL, jnp.float32))
    top = score(qi, top, True)

    def expo(j, total):
        rows = pl.ds(pl.multiple_of(j * BLOCK, BLOCK), BLOCK)
        e = jnp.exp(s_ref[rows, :] - top)
        s_ref[rows, :] = e
        return total + jnp.sum(e, axis=0, keepdims=True)

    total = lax.fori_loop(0, qi + 1, expo, jnp.zeros((1, BLOCK), jnp.float32))
    inv_total = 1.0 / total

    def weigh(j, acc):
        rows = pl.ds(pl.multiple_of(j * BLOCK, BLOCK), BLOCK)
        p = (s_ref[rows, :] * inv_total).astype(jnp.bfloat16)
        return acc + mm(vt_ref[:, rows], p)

    acc = lax.fori_loop(0, qi + 1, weigh, jnp.zeros((vt_ref.shape[0], BLOCK), jnp.float32))
    ctx_ref[...] = acc.T.astype(jnp.bfloat16)
    lse_ref[0] = top + jnp.log(total)


def attention_forward(qkv_rows, head_dim):
    seq_len, cols = qkv_rows.shape
    heads = cols // head_dim - 2
    blocks = seq_len // BLOCK
    flops = 4 * heads * head_dim * seq_len * (seq_len + BLOCK) // 2
    return pl.pallas_call(
        functools.partial(attention_forward_kernel, head_dim ** -0.5),
        grid=(heads, blocks),
        in_specs=[pl.BlockSpec((BLOCK, head_dim), lambda h, i: (i, h)), pl.BlockSpec((seq_len, head_dim), lambda h, i: (0, heads)), pl.BlockSpec((seq_len, head_dim), lambda h, i: (0, heads + 1))],
        out_specs=[pl.BlockSpec((BLOCK, head_dim), lambda h, i: (i, h)), pl.BlockSpec((1, 1, BLOCK), lambda h, i: (h, 0, i))],
        out_shape=[jax.ShapeDtypeStruct((seq_len, heads * head_dim), jnp.bfloat16), jax.ShapeDtypeStruct((heads, 1, seq_len), jnp.float32)],
        scratch_shapes=[pltpu.VMEM((head_dim, seq_len), jnp.bfloat16), pltpu.VMEM((seq_len, BLOCK), jnp.float32)],
        compiler_params=pltpu.CompilerParams(dimension_semantics=('arbitrary', 'arbitrary'), vmem_limit_bytes=32 * 1024 * 1024),
        cost_estimate=pl.CostEstimate(flops=flops, bytes_accessed=6 * seq_len * head_dim * 2, transcendentals=heads * seq_len * seq_len // 2),
        name='attn_fwd',
    )(qkv_rows, qkv_rows, qkv_rows)


def attention_backward_kernel(scale, heads, q_ref, k_ref, v_ref, g_ref, lse_ref, out_ref, kt_ref, p_ref, dp_ref, dk_ref, dv_ref):
    head, qi = pl.program_id(0), pl.program_id(1)
    head_dim = q_ref.shape[1]

    @pl.when((head == 0) & (qi == 0))
    def _():
        kt_ref[...] = k_ref[...].T
        dk_ref[...] = jnp.zeros_like(dk_ref)
        dv_ref[...] = jnp.zeros_like(dv_ref)

    q, g, lse = q_ref[...], g_ref[...], lse_ref[0]

    def first(j, delta, diagonal):
        rows = pl.ds(pl.multiple_of(j * BLOCK, BLOCK), BLOCK)
        s = mm(k_ref[rows, :], q, NT) * scale
        if diagonal:
            s = causal_fill(s)
        p = jnp.exp(s - lse)
        dp = mm(v_ref[rows, :], g, NT)
        p_ref[rows, :] = p
        dp_ref[rows, :] = dp
        dv_ref[rows, :] += mm(p.astype(jnp.bfloat16), g)
        return delta + jnp.sum(p * dp, axis=0, keepdims=True)

    delta = lax.fori_loop(0, qi, lambda j, d: first(j, d, False), jnp.zeros((1, BLOCK), jnp.float32))
    delta = first(qi, delta, True)

    def second(j, acc):
        rows = pl.ds(pl.multiple_of(j * BLOCK, BLOCK), BLOCK)
        ds = (p_ref[rows, :] * (dp_ref[rows, :] - delta) * scale).astype(jnp.bfloat16)
        dk_ref[rows, :] += mm(ds, q)
        return acc + mm(kt_ref[:, rows], ds)

    acc = lax.fori_loop(0, qi + 1, second, jnp.zeros((head_dim, BLOCK), jnp.float32))
    rows = pl.ds(pl.multiple_of(qi * BLOCK, BLOCK), BLOCK)
    for h in range(heads):
        @pl.when(head == h)
        def _():
            out_ref[rows, h * head_dim:(h + 1) * head_dim] = acc.T.astype(jnp.bfloat16)

    @pl.when((head == heads - 1) & (qi == pl.num_programs(1) - 1))
    def _():
        out_ref[:, heads * head_dim:(heads + 1) * head_dim] = dk_ref[...].astype(jnp.bfloat16)
        out_ref[:, (heads + 1) * head_dim:] = dv_ref[...].astype(jnp.bfloat16)


def attention_backward(grad_ctx, qkv_rows, log_sum, head_dim):
    seq_len, cols = qkv_rows.shape
    heads = cols // head_dim - 2
    blocks = seq_len // BLOCK
    flops = 10 * heads * head_dim * seq_len * (seq_len + BLOCK) // 2
    return pl.pallas_call(
        functools.partial(attention_backward_kernel, head_dim ** -0.5, heads),
        grid=(heads, blocks),
        in_specs=[pl.BlockSpec((BLOCK, head_dim), lambda h, i: (i, h)), pl.BlockSpec((seq_len, head_dim), lambda h, i: (0, heads)), pl.BlockSpec((seq_len, head_dim), lambda h, i: (0, heads + 1)), pl.BlockSpec((BLOCK, head_dim), lambda h, i: (i, h)), pl.BlockSpec((1, 1, BLOCK), lambda h, i: (h, 0, i))],
        out_specs=pl.BlockSpec((seq_len, cols), lambda h, i: (0, 0)),
        out_shape=jax.ShapeDtypeStruct((seq_len, cols), jnp.bfloat16),
        scratch_shapes=[pltpu.VMEM((head_dim, seq_len), jnp.bfloat16), pltpu.VMEM((seq_len, BLOCK), jnp.float32), pltpu.VMEM((seq_len, BLOCK), jnp.float32), pltpu.VMEM((seq_len, head_dim), jnp.float32), pltpu.VMEM((seq_len, head_dim), jnp.float32)],
        compiler_params=pltpu.CompilerParams(dimension_semantics=('arbitrary', 'arbitrary'), vmem_limit_bytes=48 * 1024 * 1024),
        cost_estimate=pl.CostEstimate(flops=flops, bytes_accessed=12 * seq_len * head_dim * 2, transcendentals=heads * seq_len * seq_len // 2),
        name='attn_bwd',
    )(qkv_rows, qkv_rows, qkv_rows, grad_ctx, log_sum)


def gather_rows(values):
    return lax.all_gather(values, 'tp', axis=0, tiled=True)


def scatter_rows(values):
    return lax.psum_scatter(values, 'tp', scatter_dimension=0, tiled=True)


def tied(value, *after):
    return lax.optimization_barrier((value,) + after)[0]


def swap_dp(values):
    return lax.ppermute(values, 'dp', [(0, 1), (1, 0)])


def swap_tp(values, flip):
    return lax.ppermute(values, 'tp', [(i, i ^ flip) for i in range(lax.axis_size('tp'))])


def fetch_peer(chunks):
    mine = jnp.where(lax.axis_index('tp') % 2 == 0, chunks[0], chunks[1])
    first = swap_dp(mine)
    second = swap_tp(first, 1)
    return first, second


def dp_half(values, axis, index):
    size = values.shape[axis] // 2
    return lax.dynamic_slice_in_dim(values, index * size, size, axis=axis)


def layer_half(weights, layer, axis, index):
    sizes = list(weights.shape[1:])
    sizes[axis] //= 2
    starts = [layer, 0, 0]
    starts[1 + axis] = index * sizes[axis]
    return lax.dynamic_slice(weights, starts, [1] + sizes)[0]


def gate_parts(gate_pre, up_pre, grad_act):
    gate_sig = jax.nn.sigmoid(gate_pre)
    gate_act = gate_pre * gate_sig
    hidden_act = (gate_act * up_pre).astype(jnp.bfloat16)
    grad_gate_pre = (grad_act * up_pre * gate_sig * (1.0 + gate_pre * (1.0 - gate_sig))).astype(jnp.bfloat16)
    grad_up_pre = (grad_act * gate_act).astype(jnp.bfloat16)
    return hidden_act, grad_gate_pre, grad_up_pre


def gather_wout(shard, dp_me):
    mine = dp_half(shard, 0, dp_me)
    got = swap_tp(mine, 2)
    other = swap_dp(got)
    far = jnp.concatenate([jnp.where(dp_me == 0, got, other), jnp.where(dp_me == 0, other, got)], axis=0)
    near = jnp.concatenate([shard, far], axis=0)
    core = swap_tp(near, 1)
    return jnp.concatenate([near, core], axis=0)


def heads_to_rows(context):
    me, ways = lax.axis_index('tp'), lax.axis_size('tp')
    rows = context.shape[0] // ways
    pieces = []
    for flip in (0, 2, 1, 3):
        piece = lax.dynamic_slice_in_dim(context, (me ^ flip) * rows, rows, axis=0)
        pieces.append(swap_tp(piece, flip) if flip else piece)
    return jnp.concatenate(pieces, axis=1)


def replica_sum(values):
    for axis in ('dp', 'tp'):
        ways = lax.axis_size(axis)
        step = 1
        while step < ways:
            values = values + lax.ppermute(values, axis, [(i, i ^ step) for i in range(ways)])
            step *= 2
    return values


def row_chunks(values, count=2):
    return jnp.split(values, count, axis=0)


def device_step(hidden, out_grad, gain_attn, w_qkv, w_out, gain_mlp, w_gate, w_up, w_down):
    layer_count, kv_local, group_cols = w_qkv.shape[0], w_qkv.shape[2], w_qkv.shape[3]
    head_dim = (group_cols - w_out.shape[1] // kv_local) // 2
    w_qkv = w_qkv.reshape(layer_count, w_qkv.shape[1], kv_local * group_cols)
    dp_me = lax.axis_index('dp')
    resid_rows = hidden[0]
    kept_state = []
    full_wout = None
    for l in range(layer_count):
        normed, inv_one = rms_forward(resid_rows, gain_attn[l])
        full_normed = gather_rows(normed)
        if full_wout is None:
            full_wout = gather_wout(tied(w_out[l], full_normed), dp_me)
        qkv_rows = mm(full_normed, w_qkv[l]).astype(jnp.bfloat16)
        context, log_sum = attention_forward(qkv_rows, head_dim)
        attn_rows = mm(heads_to_rows(context), full_wout)
        mid_resid = (resid_rows.astype(jnp.float32) + attn_rows).astype(jnp.bfloat16)
        normed_mlp, inv_two = rms_forward(mid_resid, gain_mlp[l])
        kept_state.append((resid_rows, inv_one, normed, qkv_rows, context, log_sum, mid_resid, inv_two, normed_mlp))
        if l + 1 < layer_count:
            full_mlp = [gather_rows(rows) for rows in row_chunks(normed_mlp, FWD_CHUNKS)]
            full_wout = gather_wout(tied(w_out[l + 1], full_mlp[-1]), dp_me)
            scattered, part = [], None
            for rows in full_mlp:
                if part is not None:
                    rows = tied(rows, part)
                gate_pre = mm(rows, w_gate[l])
                up_pre = mm(rows, w_up[l])
                hidden_act = (jax.nn.silu(gate_pre) * up_pre).astype(jnp.bfloat16)
                part = mm(hidden_act, w_down[l])
                scattered.append(scatter_rows(part))
            resid_rows = (mid_resid.astype(jnp.float32) + jnp.concatenate(scattered, axis=0)).astype(jnp.bfloat16)
    grad_resid = out_grad[0]
    outs = {name: [None] * layer_count for name in ('qkv', 'out', 'gate', 'up', 'down', 'gain_one', 'gain_two')}
    after = None
    for l in reversed(range(layer_count)):
        resid_rows, inv_one, normed, qkv_rows, context, log_sum, mid_resid, inv_two, normed_mlp = kept_state[l]
        last = l + 1 == layer_count
        grad_parts = row_chunks(grad_resid)
        mlp_parts = row_chunks(normed_mlp if last else tied(normed_mlp, after))
        if last:
            grad_parts = [tied(rows, normed_mlp) for rows in grad_parts]
        mlp_rows, grad_rows = [], []
        for c in range(2):
            mlp_rows.append(gather_rows(mlp_parts[c]))
            grad_rows.append(gather_rows(grad_parts[c]))
        peer_grad = fetch_peer(grad_rows)
        peer_mlp = fetch_peer(mlp_rows)
        halves, scattered, part = [], [], None
        for c in range(2):
            rows = grad_rows[c] if part is None else tied(grad_rows[c], part)
            gate_pre = mm(mlp_rows[c], w_gate[l])
            up_pre = mm(mlp_rows[c], w_up[l])
            grad_act = mm(rows, w_down[l], NT)
            hidden_act, grad_gate_pre, grad_up_pre = gate_parts(gate_pre, up_pre, grad_act)
            part = mm(grad_gate_pre, w_gate[l], NT) + mm(grad_up_pre, w_up[l], NT)
            scattered.append(scatter_rows(tied(part, scattered[0]) if c else part))
            halves.append((hidden_act, grad_gate_pre, grad_up_pre))
        acts, gates, ups = zip(*halves)
        own_rows, own_grad = [tied(r, part) for r in mlp_rows], [tied(r, part) for r in grad_rows]
        sum_gate = sum(mm(r, dp_half(v, 1, dp_me), TN) for r, v in zip(own_rows, gates))
        sum_up = sum(mm(r, dp_half(v, 1, dp_me), TN) for r, v in zip(own_rows, ups))
        sum_down = sum(mm(dp_half(v, 1, dp_me), r, TN) for r, v in zip(own_grad, acts))
        gate_half, up_half, down_half = layer_half(w_gate, l, 1, dp_me), layer_half(w_up, l, 1, dp_me), layer_half(w_down, l, 0, dp_me)

        def peer_parts(m, g):
            gate_pre, up_pre = mm(m, gate_half), mm(m, up_half)
            grad_act = mm(g, down_half, NT)
            return gate_parts(gate_pre, up_pre, grad_act)

        scattered = tied(scattered, sum_gate, sum_up, sum_down)
        grad_mid, outs['gain_two'][l] = rms_backward(jnp.concatenate(scattered, axis=0), mid_resid, inv_two, gain_mlp[l])
        grad_mid = (grad_mid + grad_resid.astype(jnp.float32)).astype(jnp.bfloat16)
        full_grad_mid = gather_rows(grad_mid)
        first_mlp, first_grad = tied(peer_mlp[0], grad_mid), tied(peer_grad[0], grad_mid)
        first_values = peer_parts(first_mlp, first_grad)
        sum_down = sum_down + mm(first_values[0], tied(peer_grad[0], grad_mid), TN)
        full_grad_mid = tied(full_grad_mid, sum_down)
        their_wout = mm(dp_half(context, 1, 1 - dp_me), full_grad_mid, TN)
        got_wout = swap_dp(their_wout)
        grad_ctx = mm(full_grad_mid, w_out[l], NT).astype(jnp.bfloat16)
        grad_qkv = attention_backward(grad_ctx, qkv_rows, log_sum, head_dim)
        grad_attn_part = mm(grad_qkv, w_qkv[l], NT)
        grad_normed = scatter_rows(grad_attn_part)
        if not last:
            full_normed = gather_rows(tied(normed, full_grad_mid))
        full_normed, late_grad_mid, first_values, second_mlp, second_grad = tied((full_normed, full_grad_mid, first_values, peer_mlp[1], peer_grad[1]), grad_attn_part)
        their_wqkv = mm(full_normed, dp_half(grad_qkv, 1, 1 - dp_me), TN)
        got_wqkv = swap_dp(their_wqkv)
        my_wqkv = mm(full_normed, dp_half(grad_qkv, 1, dp_me), TN)
        my_wout = mm(dp_half(context, 1, dp_me), late_grad_mid, TN)
        after = my_wqkv
        first_values, second_mlp, second_grad = tied((first_values, second_mlp, second_grad), my_wqkv, my_wout)
        second_values = peer_parts(second_mlp, second_grad)
        outs['down'][l] = (sum_down + mm(second_values[0], peer_grad[1], TN)).astype(jnp.bfloat16)
        outs['gate'][l] = (sum_gate + sum(mm(r, v[1], TN) for r, v in zip(peer_mlp, (first_values, second_values)))).astype(jnp.bfloat16)
        outs['up'][l] = (sum_up + sum(mm(r, v[2], TN) for r, v in zip(peer_mlp, (first_values, second_values)))).astype(jnp.bfloat16)
        late = (outs['gate'][l], outs['up'][l], outs['down'][l])
        grad_normed = tied(grad_normed, *late)
        got_wout = tied(got_wout, *late)
        got_wqkv = tied(got_wqkv, *late)
        grad_in, outs['gain_one'][l] = rms_backward(grad_normed, resid_rows, inv_one, gain_attn[l])
        grad_resid = (grad_in + grad_mid.astype(jnp.float32)).astype(jnp.bfloat16)
        if last:
            got_wqkv = tied(got_wqkv, grad_resid)
            got_wout = tied(got_wout, grad_resid)
        outs['qkv'][l] = (my_wqkv + got_wqkv).astype(jnp.bfloat16).reshape(my_wqkv.shape[0], kv_local, -1)
        outs['out'][l] = (my_wout + got_wout).astype(jnp.bfloat16)
    gain_sums = replica_sum(jnp.stack([jnp.stack(outs['gain_one']), jnp.stack(outs['gain_two'])]))
    stacked = {name: jnp.stack(outs[name]) for name in ('qkv', 'out', 'gate', 'up', 'down')}
    return (grad_resid[None], gain_sums[0], stacked['qkv'], stacked['out'], gain_sums[1], stacked['gate'], stacked['up'], stacked['down'])


def solution(mesh):
    return jax.shard_map(device_step, mesh=mesh, in_specs=IN_SPECS, out_specs=OUT_SPECS, check_vma=False)
```
